32 devices in a mesh: row: 16 (over z, x, core), blk: 2 (over y).
Axes of the slice: x: 2, y: 2, z: 4, core: 2. Of those that a mesh axis runs over, the one named last changes fastest.
Arguments:
- embeddings: bfloat16 [8192, 192], P(('row', 'blk')), may hold values from -30 to 30
- vectors: float32 [8192, 16], P(('row', 'blk')), may hold values from -6 to 6
Outputs:
- basis: float32 [8192, 16], P(('row', 'blk'))
- triangle: float32 [16, 16], replicated
The draws below stay inside these ranges and needn't reach their ends.
All inputs are finite; a program needn't handle non-finite values.
Results may differ from the reference program's by a relative error of at most 0.0088.
Values may be sent and summed in bfloat16 or wider, within the bound.
A program may use at most 64 MiB of HBM per device.

```python
import math
import jax
import jax.numpy as jnp
from jax import lax

DIM = 192
VEC = 16
SEGMENTS = 8192


voices = 48


rooms = 4


def draw_embeddings(key, part):
    keys = jax.random.split(jax.random.fold_in(key, 11), 7)
    labels = jax.random.randint(keys[0], (SEGMENTS,), 0, voices)
    places = jax.random.randint(keys[1], (SEGMENTS,), 0, rooms)
    centres = jax.random.normal(keys[2], (voices, DIM), jnp.float32)
    room_dirs = jax.random.normal(keys[3], (rooms, DIM), jnp.float32)
    strength = jax.random.uniform(keys[4], (SEGMENTS, 1), jnp.float32, 0.2, 1.5)
    channel = jax.random.uniform(keys[5], (SEGMENTS, 1), jnp.float32, 0.0, 1.0)
    noise = jax.random.normal(keys[6], (SEGMENTS, DIM), jnp.float32)
    values = 1.5 * strength * centres[labels] + channel * room_dirs[places] + noise
    return jnp.clip(values, -30.0, 30.0).astype(jnp.bfloat16)


def draw_vectors(key, part):
    first, second, third = jax.random.split(jax.random.fold_in(key, 23), 3)
    signs = jnp.where(jax.random.bernoulli(second, 0.5, (VEC,)), 1.0, -1.0)
    offsets = jax.random.uniform(first, (VEC,), jnp.float32, 0.5, 1.0) * signs
    noise = jnp.clip(jax.random.normal(third, (SEGMENTS, VEC), jnp.float32), -4.0, 4.0)
    return jnp.clip(noise + offsets[None, :], -6.0, 6.0)


def setup_inputs(seed: int = 0) -> dict:
    arg_keys = jax.random.split(jax.random.key(seed), 3)
    return {
        "embeddings": draw_embeddings(jax.random.fold_in(arg_keys[2], 71), 0),
        "vectors": draw_vectors(jax.random.fold_in(arg_keys[2], 71), 0),
    }


sharpness = 10.0
epsilon = 1e-06

def normalize(embeddings):
    values = embeddings.astype(jnp.float32)
    return (values * lax.rsqrt(lax.optimization_barrier(jnp.sum(values * values, axis=1, keepdims=True)) + epsilon)).astype(jnp.bfloat16)

def affinity(block_rows, columns):
    scores = lax.dot_general(block_rows.astype(jnp.float32), columns.astype(jnp.float32), (((1,), (1,)), ((), ())), preferred_element_type=jnp.float32)
    return jnp.exp(sharpness * (scores - 1.0))

def reference(embeddings, vectors):
    unit_rows = normalize(embeddings)
    total = unit_rows.shape[0]
    blocks = unit_rows.reshape(-1, math.gcd(total, 512), unit_rows.shape[1])

    def degree_block(block_rows):
        return lax.optimization_barrier(jnp.sum(affinity(block_rows, unit_rows), axis=1))
    degree = lax.map(degree_block, blocks).reshape(total)
    inverse_root = lax.rsqrt(degree)
    weighted = (vectors * inverse_root[:, None]).astype(jnp.bfloat16)

    def apply_block(block_rows):
        tile = affinity(block_rows, unit_rows).astype(jnp.bfloat16)
        return jnp.dot(tile.astype(jnp.float32), weighted.astype(jnp.float32), preferred_element_type=jnp.float32)
    summed = lax.map(apply_block, blocks).reshape(total, vectors.shape[1])
    projected = summed * inverse_root[:, None]
    gram_matrix = jnp.dot(projected.T, projected, precision=lax.Precision.HIGHEST)
    factor = jnp.linalg.cholesky(gram_matrix)
    basis = jax.scipy.linalg.solve_triangular(factor, projected.T, lower=True).T
    return (basis, factor.T)
```

```python
import functools
import math

import jax
import jax.numpy as jnp
from jax import lax
from jax.experimental import pallas as pl
from jax.experimental.pallas import tpu as pltpu
from jax.sharding import PartitionSpec as P

sharpness = 10.0
epsilon = 1e-06
scale2 = sharpness * math.log2(math.e)
MESH = pl.DeviceIdType.MESH
HIGH = lax.Precision.HIGHEST
TRANS = (((1,), (1,)), ((), ()))


def flip(bit, by):
    return bit + by - 2 * bit * by


def swap(x, bit):
    if bit == 4:
        return pltpu.roll(x, 4, 0)
    row = lax.broadcasted_iota(jnp.int32, x.shape, 0)
    return jnp.where((row & bit) == 0, pltpu.roll(x, 8 - bit, 0), pltpu.roll(x, bit, 0))


def pair_sum(x):
    while x.shape[0] > 1:
        x = x.reshape(x.shape[0] // 2, 2, *x.shape[1:])
        x = x[:, 0] + x[:, 1]
    return x[0]


def kernel(plane_line, emb_hbm, vec_hbm, basis_ref, tri_ref, emb_ref, in_sem,
           rows, cols, turned, aff, vecs, dpart, dsend, drecv, wts, spart, srecv, gsend, grecv,
           row_s, row_r, col_s, col_r, vec_s, vec_r, deg_s, deg_r, sum_s, sum_r, g_s, g_r):
    blk_low, line = plane_line
    n_local = emb_ref.shape[1]
    k = vecs.shape[1]
    r = lax.axis_index("row")
    b = lax.axis_index("blk")
    core, x, y = r % 2, (r // 2) % 2, b % 2
    z = (r // 4) * blk_low + b // 2

    def toggled(s):
        total, unit_bit = 0, 1
        while unit_bit < line:
            total = total + unit_bit * flip((z // unit_bit) % 2, (s // unit_bit) % 2)
            unit_bit *= 2
        return total

    def peer(s, t):
        c2 = flip(core, t % 2)
        x2 = flip(x, (t // 2) % 2)
        y2 = flip(y, (t // 4) % 2)
        z2 = toggled(s)
        return ((z2 // blk_low) * 4 + x2 * 2 + c2, (z2 % blk_low) * 2 + y2)

    def mate(t):
        return peer(0, t)

    def along(s):
        return peer(s, 0)

    emb_in = pltpu.make_async_copy(emb_hbm, emb_ref, in_sem.at[0])
    vec_in = pltpu.make_async_copy(vec_hbm, vecs.at[0], in_sem.at[1])
    emb_in.start()
    vec_in.start()
    barrier = pltpu.get_barrier_semaphore()
    for t in range(1, 8):
        pl.semaphore_signal(barrier, inc=1, device_id=mate(t), device_id_type=MESH)
    for s in range(1, line):
        pl.semaphore_signal(barrier, inc=1, device_id=along(s), device_id_type=MESH)

    emb_in.wait()
    values = emb_ref[...].astype(jnp.float32)
    norm = lax.rsqrt(jnp.sum(values * values, axis=0, keepdims=True) + epsilon)
    unit = (values * norm).astype(jnp.bfloat16)
    rows[0] = unit
    cols[0] = unit
    vec_in.wait()
    pl.semaphore_wait(barrier, 7 + line - 1)

    def send(src, dst, ssem, rsem, to):
        copy = pltpu.make_async_remote_copy(
            src_ref=src, dst_ref=dst, send_sem=ssem, recv_sem=rsem, device_id=to, device_id_type=MESH)
        copy.start()
        return copy

    row_copy = {}
    col_copy = {}
    vec_copy = {}
    order = list(range(1, line))
    relayed = line == 4
    half = cols.shape[1] // 2

    def send_row(t, source=0, to=None):
        row_copy[t] = send(rows.at[source], rows.at[t], row_s.at[t], row_r.at[t], mate(t if to is None else to))

    def send_vec(t, source=0, to=None):
        vec_copy[t] = send(vecs.at[source], vecs.at[t], vec_s.at[t], vec_r.at[t], mate(t if to is None else to))

    def send_part(key, source, slot, start, to):
        part = pl.ds(start, half)
        col_copy[key] = send(cols.at[source, part], cols.at[slot, part], col_s.at[key], col_r.at[key], to)

    send_row(1)
    for t in (2, 4, 6):
        send_row(t)
    if relayed:
        send_part(2, 0, 2, 0, along(2))
        send_part(4, 0, 2, half, along(2))
        col_copy[1] = send(cols.at[0], cols.at[1], col_s.at[1], col_r.at[1], along(1))
        send_part(3, 0, 3, half, along(3))
    else:
        for s in order:
            col_copy[s] = send(cols.at[0], cols.at[s], col_s.at[s], col_r.at[s], along(s))
    for t in (1, 2, 4, 6):
        send_vec(t)

    def tile(s, t):
        scores = jnp.dot(turned[s], rows[t], preferred_element_type=jnp.float32)
        e = jnp.exp2(scores * scale2 - scale2)
        aff[s, t] = e.astype(jnp.bfloat16)
        return jnp.sum(e.reshape(n_local // 8, 8, n_local), axis=0)

    def turn(s):
        turned[s] = cols[s].astype(jnp.float32).T.astype(jnp.bfloat16)

    have_rows, have_cols = [], []

    def do_tile(s, t):
        if len(have_cols) == 1:
            dpart[t] = tile(s, t)
        else:
            dpart[t] = dpart[t] + tile(s, t)

    def row_here(t):
        if t:
            row_copy[t].wait_recv()
            if t in (2, 4, 6):
                send_row(t + 1, source=t, to=1)
        have_rows.append(t)
        for s in have_cols:
            if s == 0:
                dpart[t] = tile(0, t)
            else:
                dpart[t] = dpart[t] + tile(s, t)

    def col_here(s):
        turn(s)
        have_cols.append(s)
        for t in have_rows:
            dpart[t] = dpart[t] + tile(s, t)

    turn(0)
    have_cols.append(0)
    row_here(0)
    if relayed:
        row_here(1)
        row_here(2)
        row_here(4)
        col_copy[2].wait_recv()
        send_part(5, 2, 3, 0, along(1))
        row_here(3)
        row_here(5)
        col_copy[1].wait_recv()
        col_here(1)
        row_here(6)
        col_copy[4].wait_recv()
        col_here(2)
        row_here(7)
        col_copy[3].wait_recv()
        col_copy[5].wait_recv()
        col_here(3)
    else:
        for t in (1, 2, 4, 6, 3, 5, 7):
            row_here(t)
        for s in order:
            col_copy[s].wait_recv()
            turn(s)

            def body(t, carry):
                dpart[t] = dpart[t] + tile(s, t)
                return carry

            lax.fori_loop(0, 8, body, 0)

    dsend[...] = jnp.concatenate([jnp.sum(dpart[t], axis=0, keepdims=True) for t in range(8)], axis=0)
    deg_copy = {}
    for t in (7, 6, 5, 4, 3, 2, 1):
        deg_copy[t] = send(dsend, drecv.at[t], deg_s.at[t], deg_r.at[t], mate(t))
    for t in (2, 4, 6):
        vec_copy[t].wait_recv()
        send_vec(t + 1, source=t, to=1)
    parts = [dsend[...]]
    for t in range(1, 8):
        deg_copy[t].wait_recv()
        parts.append(drecv[t])
    for bit in (1, 2, 4):
        parts = [parts[i] + swap(parts[i + 1], bit) for i in range(0, len(parts), 2)]
    inverse_root = lax.rsqrt(parts[0])
    for t in (1, 3, 5, 7):
        vec_copy[t].wait_recv()
    for t in range(8):
        wts[:, t * n_local:(t + 1) * n_local] = (vecs[t] * inverse_root[t:t + 1, :]).astype(jnp.bfloat16)

    def image(s):
        total = None
        for t in range(8):
            part = lax.dot_general(aff[s, t], wts[:, t * n_local:(t + 1) * n_local], TRANS,
                                   preferred_element_type=jnp.float32)
            total = part if total is None else total + part
        return total.T

    sum_copy = {}
    for s in reversed(order):
        spart[s] = image(s)
        sum_copy[s] = send(spart.at[s], srecv.at[s], sum_s.at[s], sum_r.at[s], along(s))
    terms = [image(0)]
    for s in order:
        sum_copy[s].wait_recv()
        terms.append(srecv[s])
    while len(terms) > 1:
        terms = [terms[i] + terms[i + 1] for i in range(0, len(terms), 2)]
    projected = terms[0] * inverse_root[0:1, :]
    gram = lax.dot_general(projected, projected, TRANS, precision=HIGH, preferred_element_type=jnp.float32)
    wide = jnp.concatenate([gram, jnp.zeros((k, 128 - k), jnp.float32)], axis=1)
    wide = jnp.concatenate([pltpu.roll(wide[h:h + 8], 0, 1, stride=k, stride_axis=0) for h in (0, 8)], axis=0)
    gsend[...] = jnp.sum(wide.reshape(2, 8, 128), axis=1)
    grecv[0] = gsend[...]
    g_copy = {}
    for s in reversed(range(line)):
        for t in reversed(range(8)):
            if s or t:
                i = s * 8 + t
                g_copy[i] = send(gsend, grecv.at[i], g_s.at[i], g_r.at[i], peer(s, t))
    for i in range(1, 8 * line):
        g_copy[i].wait_recv()
    total = pair_sum(grecv[...])
    lane = lax.broadcasted_iota(jnp.int32, (16, 128), 1)
    below = lax.broadcasted_iota(jnp.int32, (16, 128), 0)
    flat = jnp.concatenate([jnp.broadcast_to(total[h:h + 1], (8, 128)) for h in (0, 1)], axis=0)
    square = [pltpu.roll(flat[h:h + 8], k, 1, stride=k, stride_axis=0) for h in (0, 8)]
    square = jnp.concatenate([swap(swap(swap(q, 1), 2), 4) for q in square], axis=0)
    a = [jnp.broadcast_to(square[:, j:j + 1], (16, 128)) for j in range(k)]
    m = projected
    pivot = jnp.zeros((16, 128), jnp.float32)
    for i in range(k):
        head = a[i][i:i + 1]
        pivot = jnp.where(below == i, head, pivot)
        f = jnp.where(below > i, a[i] * (1.0 / head), 0.0)
        for j in range(i + 1, k):
            a[j] = a[j] - f * a[j][i:i + 1]
        m = m - jnp.concatenate([f] * (n_local // 128), axis=1) * m[i:i + 1]
    root = lax.rsqrt(pivot)
    tri = jnp.zeros((16, 128), jnp.float32)
    for j in range(k):
        tri = jnp.where((lane == j) & (below <= j), a[j], tri)
    tri_ref[...] = (tri * root)[:, :k]
    basis_ref[...] = m * jnp.concatenate([root] * (n_local // 128), axis=1)

    for group in (row_copy, col_copy, vec_copy, deg_copy, sum_copy, g_copy):
        for copy in group.values():
            copy.wait_send()


def per_device(sizes, embeddings, vectors):
    blk_low, line = sizes
    n, dim = embeddings.shape
    k = vectors.shape[1]
    dma = pltpu.SemaphoreType.DMA
    vmem = pl.BlockSpec(memory_space=pltpu.VMEM)
    basis_t, tri = pl.pallas_call(
        functools.partial(kernel, sizes),
        out_shape=(jax.ShapeDtypeStruct((k, n), jnp.float32), jax.ShapeDtypeStruct((k, k), jnp.float32)),
        in_specs=[pl.BlockSpec(memory_space=pltpu.HBM)] * 2,
        out_specs=(vmem, vmem),
        scratch_shapes=[
            pltpu.VMEM((dim, n), jnp.bfloat16),
            dma((2,)),
            pltpu.VMEM((8, dim, n), jnp.bfloat16),
            pltpu.VMEM((line, dim, n), jnp.bfloat16),
            pltpu.VMEM((line, n, dim), jnp.bfloat16),
            pltpu.VMEM((line, 8, n, n), jnp.bfloat16),
            pltpu.VMEM((8, k, n), jnp.float32),
            pltpu.VMEM((8, 8, n), jnp.float32),
            pltpu.VMEM((8, n), jnp.float32),
            pltpu.VMEM((8, 8, n), jnp.float32),
            pltpu.VMEM((k, 8 * n), jnp.bfloat16),
            pltpu.VMEM((line, k, n), jnp.float32),
            pltpu.VMEM((line, k, n), jnp.float32),
            pltpu.VMEM((2, 128), jnp.float32),
            pltpu.VMEM((8 * line, 2, 128), jnp.float32),
            dma((8,)), dma((8,)), dma((line + 2,)), dma((line + 2,)), dma((8,)), dma((8,)),
            dma((8,)), dma((8,)), dma((line,)), dma((line,)), dma((8 * line,)), dma((8 * line,)),
        ],
        compiler_params=pltpu.CompilerParams(
            collective_id=0, has_side_effects=True, vmem_limit_bytes=(16 if line <= 8 else 60) * 1024 * 1024),
        name="cluster",
    )(embeddings.T, vectors.T)
    return basis_t.T, tri


def solution(mesh):
    blk_low = mesh.shape["blk"] // 2
    line = (mesh.shape["row"] // 4) * blk_low
    placed = (P(("row", "blk"), None), P(("row", "blk"), None))
    return jax.shard_map(
        functools.partial(per_device, (blk_low, line)),
        mesh=mesh,
        in_specs=placed,
        out_specs=(P(("row", "blk"), None), P()),
        check_vma=False,
    )
```

```python
import functools
import math

import jax
import jax.numpy as jnp
from jax import lax
from jax.experimental import pallas as pl
from jax.experimental.pallas import tpu as pltpu
from jax.sharding import PartitionSpec as P

sharpness = 10.0
epsilon = 1e-06
scale2 = sharpness * math.log2(math.e)
MESH = pl.DeviceIdType.MESH
TRANS = (((1,), (1,)), ((), ()))


def flip(bit, by):
    return bit + by - 2 * bit * by


def swap(x, bit):
    if bit == 4:
        return pltpu.roll(x, 4, 0)
    row = lax.broadcasted_iota(jnp.int32, x.shape, 0)
    return jnp.where((row & bit) == 0, pltpu.roll(x, 8 - bit, 0), pltpu.roll(x, bit, 0))


def split(x):
    high = x.astype(jnp.bfloat16)
    rest = x - high.astype(jnp.float32)
    middle = rest.astype(jnp.bfloat16)
    low = (rest - middle.astype(jnp.float32)).astype(jnp.bfloat16)
    return high, middle, low


def pair_sum(x):
    while x.shape[0] > 1:
        x = x.reshape(x.shape[0] // 2, 2, *x.shape[1:])
        x = x[:, 0] + x[:, 1]
    return x[0]


def kernel(plane_line, emb_hbm, vec_hbm, basis_ref, tri_ref, emb_ref, in_sem,
           rows, cols, turned, aff, vecs, dpart, dsend, drecv, wts, spart, srecv, gsend, grecv,
           row_s, row_r, col_s, col_r, vec_s, vec_r, deg_s, deg_r, sum_s, sum_r, g_s, g_r):
    blk_low, line = plane_line
    n_local = emb_ref.shape[1]
    k = vecs.shape[1]
    r = lax.axis_index("row")
    b = lax.axis_index("blk")
    core, x, y = r % 2, (r // 2) % 2, b % 2
    z = (r // 4) * blk_low + b // 2

    def toggled(s):
        total, unit_bit = 0, 1
        while unit_bit < line:
            total = total + unit_bit * flip((z // unit_bit) % 2, (s // unit_bit) % 2)
            unit_bit *= 2
        return total

    def peer(s, t):
        c2 = flip(core, t % 2)
        x2 = flip(x, (t // 2) % 2)
        y2 = flip(y, (t // 4) % 2)
        z2 = toggled(s)
        return ((z2 // blk_low) * 4 + x2 * 2 + c2, (z2 % blk_low) * 2 + y2)

    def mate(t):
        return peer(0, t)

    def along(s):
        return peer(s, 0)

    emb_in = pltpu.make_async_copy(emb_hbm, emb_ref, in_sem.at[0])
    vec_in = pltpu.make_async_copy(vec_hbm, vecs.at[0], in_sem.at[1])
    emb_in.start()
    vec_in.start()
    barrier = pltpu.get_barrier_semaphore()
    for t in range(1, 8):
        pl.semaphore_signal(barrier, inc=1, device_id=mate(t), device_id_type=MESH)
    for s in range(1, line):
        pl.semaphore_signal(barrier, inc=1, device_id=along(s), device_id_type=MESH)

    emb_in.wait()
    values = emb_ref[...].astype(jnp.float32)
    norm = lax.rsqrt(jnp.sum(values * values, axis=0, keepdims=True) + epsilon)
    unit = (values * norm).astype(jnp.bfloat16)
    rows[0] = unit
    cols[0] = unit
    vec_in.wait()
    pl.semaphore_wait(barrier, 7 + line - 1)

    def send(src, dst, ssem, rsem, to):
        copy = pltpu.make_async_remote_copy(
            src_ref=src, dst_ref=dst, send_sem=ssem, recv_sem=rsem, device_id=to, device_id_type=MESH)
        copy.start()
        return copy

    row_copy = {}
    col_copy = {}
    vec_copy = {}
    order = list(range(1, line))
    relayed = line == 4
    half = n_local // 2

    def send_row(t, source=0, to=None):
        row_copy[t] = send(rows.at[source], rows.at[t], row_s.at[t], row_r.at[t], mate(t if to is None else to))

    def send_vec(t, source=0, to=None):
        vec_copy[t] = send(vecs.at[source], vecs.at[t], vec_s.at[t], vec_r.at[t], mate(t if to is None else to))

    def send_part(key, source, slot, start, to):
        part = pl.ds(start, half)
        col_copy[key] = send(cols.at[source, :, part], cols.at[slot, :, part], col_s.at[key], col_r.at[key], to)

    if relayed:
        send_part(2, 0, 2, 0, along(2))
        send_part(4, 0, 2, half, along(2))
        col_copy[1] = send(cols.at[0], cols.at[1], col_s.at[1], col_r.at[1], along(1))
        send_part(3, 0, 3, half, along(3))
    else:
        for s in order:
            col_copy[s] = send(cols.at[0], cols.at[s], col_s.at[s], col_r.at[s], along(s))
    for t in (2, 4, 6, 1):
        send_row(t)
    for t in (1, 2, 4, 6):
        send_vec(t)

    def tile(s, t):
        scores = jnp.dot(turned[s], rows[t], preferred_element_type=jnp.float32)
        e = jnp.exp2(scores * scale2 - scale2)
        aff[s, t] = e.astype(jnp.bfloat16)
        return jnp.sum(e.reshape(n_local // 8, 8, n_local), axis=0)

    def turn(s):
        turned[s] = cols[s].astype(jnp.float32).T.astype(jnp.bfloat16)

    have_rows, have_cols = [], []

    def row_in(t):
        row_copy[t].wait_recv()
        if t in (2, 4, 6):
            send_row(t + 1, source=t, to=1)

    def row_here(t, wait=True):
        if t and wait:
            row_in(t)
        have_rows.append(t)
        for s in have_cols:
            if s == 0:
                dpart[t] = tile(0, t)
            else:
                dpart[t] = dpart[t] + tile(s, t)

    def col_here(s):
        turn(s)
        have_cols.append(s)
        for t in have_rows:
            dpart[t] = dpart[t] + tile(s, t)

    def half_here(s, start):
        part = slice(start, start + half)
        turned[s, part] = cols[s, :, part].astype(jnp.float32).T.astype(jnp.bfloat16)
        for t in range(8):
            scores = jnp.dot(turned[s, part], rows[t], preferred_element_type=jnp.float32)
            e = jnp.exp2(scores * scale2 - scale2)
            aff[s, t, part] = e.astype(jnp.bfloat16)
            dpart[t] = dpart[t] + jnp.sum(e.reshape(half // 8, 8, n_local), axis=0)

    turn(0)
    have_cols.append(0)
    row_here(0)
    if relayed:
        row_here(1)
        col_copy[2].wait_recv()
        send_part(5, 2, 3, 0, along(1))
        row_here(2)
        row_here(4)
        row_here(3)
        row_here(5)
        row_in(6)
        col_copy[1].wait_recv()
        col_here(1)
        row_here(6, False)
        col_copy[4].wait_recv()
        col_here(2)
        row_here(7)
        col_copy[3].wait_recv()
        half_here(3, half)
        col_copy[5].wait_recv()
        half_here(3, 0)
    else:
        for t in (1, 2, 4, 6, 3, 5, 7):
            row_here(t)
        for s in order:
            col_copy[s].wait_recv()
            turn(s)

            def body(t, carry):
                dpart[t] = dpart[t] + tile(s, t)
                return carry

            lax.fori_loop(0, 8, body, 0)

    dsend[...] = jnp.concatenate([jnp.sum(dpart[t], axis=0, keepdims=True) for t in range(8)], axis=0)
    deg_copy = {}
    for t in (7, 6, 5, 4, 3, 2, 1):
        deg_copy[t] = send(dsend, drecv.at[t], deg_s.at[t], deg_r.at[t], mate(t))
    for t in (2, 4, 6):
        vec_copy[t].wait_recv()
        send_vec(t + 1, source=t, to=1)
    parts = [dsend[...]]
    for t in range(1, 8):
        deg_copy[t].wait_recv()
        parts.append(drecv[t])
    for bit in (1, 2, 4):
        parts = [parts[i] + swap(parts[i + 1], bit) for i in range(0, len(parts), 2)]
    inverse_root = lax.rsqrt(parts[0])
    for t in (1, 3, 5, 7):
        vec_copy[t].wait_recv()
    for t in range(8):
        wts[:, t * n_local:(t + 1) * n_local] = (vecs[t] * inverse_root[t:t + 1, :]).astype(jnp.bfloat16)

    def image(s):
        total = None
        for t in range(8):
            part = lax.dot_general(aff[s, t], wts[:, t * n_local:(t + 1) * n_local], TRANS,
                                   preferred_element_type=jnp.float32)
            total = part if total is None else total + part
        return total.T

    sum_copy = {}
    for s in reversed(order):
        spart[s] = image(s)
        sum_copy[s] = send(spart.at[s], srecv.at[s], sum_s.at[s], sum_r.at[s], along(s))
    terms = [image(0)]
    for s in order:
        sum_copy[s].wait_recv()
        terms.append(srecv[s])
    while len(terms) > 1:
        terms = [terms[i] + terms[i + 1] for i in range(0, len(terms), 2)]
    projected = terms[0] * inverse_root[0:1, :]
    high, middle, low = split(projected)
    left = jnp.concatenate([high, high, middle, middle, high, low], axis=1)
    right = jnp.concatenate([high, middle, high, middle, low, high], axis=1)
    gram = lax.dot_general(left, right, TRANS, preferred_element_type=jnp.float32)
    wide = jnp.concatenate([gram, jnp.zeros((k, 128 - k), jnp.float32)], axis=1)
    wide = jnp.concatenate([pltpu.roll(wide[h:h + 8], 0, 1, stride=k, stride_axis=0) for h in (0, 8)], axis=0)
    gsend[...] = jnp.sum(wide.reshape(2, 8, 128), axis=1)
    grecv[0] = gsend[...]
    g_copy = {}
    for s in reversed(range(line)):
        for t in reversed(range(8)):
            if s or t:
                i = s * 8 + t
                g_copy[i] = send(gsend, grecv.at[i], g_s.at[i], g_r.at[i], peer(s, t))
    for i in range(1, 8 * line):
        g_copy[i].wait_recv()
    total = pair_sum(grecv[...])
    lane = lax.broadcasted_iota(jnp.int32, (16, 128), 1)
    below = lax.broadcasted_iota(jnp.int32, (16, 128), 0)
    flat = jnp.concatenate([jnp.broadcast_to(total[h:h + 1], (8, 128)) for h in (0, 1)], axis=0)
    square = [pltpu.roll(flat[h:h + 8], k, 1, stride=k, stride_axis=0) for h in (0, 8)]
    square = jnp.concatenate([swap(swap(swap(q, 1), 2), 4) for q in square], axis=0)
    a = [jnp.broadcast_to(square[:, j:j + 1], (16, 128)) for j in range(k)]
    m = projected
    pivot = jnp.zeros((16, 128), jnp.float32)
    for i in range(k):
        head = a[i][i:i + 1]
        pivot = jnp.where(below == i, head, pivot)
        f = jnp.where(below > i, a[i] * (1.0 / head), 0.0)
        for j in range(i + 1, k):
            a[j] = a[j] - f * a[j][i:i + 1]
        m = m - jnp.concatenate([f] * (n_local // 128), axis=1) * m[i:i + 1]
    root = lax.rsqrt(pivot)
    tri = jnp.zeros((16, 128), jnp.float32)
    for j in range(k):
        tri = jnp.where((lane == j) & (below <= j), a[j], tri)
    tri_ref[...] = (tri * root)[:, :k]
    basis_ref[...] = m * jnp.concatenate([root] * (n_local // 128), axis=1)

    for group in (row_copy, col_copy, vec_copy, deg_copy, sum_copy, g_copy):
        for copy in group.values():
            copy.wait_send()


def store(basis_ref, tri_ref, basis_hbm, tri_hbm, sem):
    copies = [pltpu.make_async_copy(basis_ref, basis_hbm, sem.at[0]),
              pltpu.make_async_copy(tri_ref, tri_hbm, sem.at[1])]
    for copy in copies:
        copy.start()
    for copy in copies:
        copy.wait()


def per_device(sizes, embeddings, vectors):
    blk_low, line = sizes
    n, dim = embeddings.shape
    k = vectors.shape[1]
    dma = pltpu.SemaphoreType.DMA
    vmem = pl.BlockSpec(memory_space=pltpu.VMEM)
    basis_t, tri = pl.pallas_call(
        functools.partial(kernel, sizes),
        out_shape=(jax.ShapeDtypeStruct((k, n), jnp.float32), jax.ShapeDtypeStruct((k, k), jnp.float32)),
        in_specs=[pl.BlockSpec(memory_space=pltpu.HBM)] * 2,
        out_specs=(vmem, vmem),
        scratch_shapes=[
            pltpu.VMEM((dim, n), jnp.bfloat16),
            dma((2,)),
            pltpu.VMEM((8, dim, n), jnp.bfloat16),
            pltpu.VMEM((line, dim, n), jnp.bfloat16),
            pltpu.VMEM((line, n, dim), jnp.bfloat16),
            pltpu.VMEM((line, 8, n, n), jnp.bfloat16),
            pltpu.VMEM((8, k, n), jnp.float32),
            pltpu.VMEM((8, 8, n), jnp.float32),
            pltpu.VMEM((8, n), jnp.float32),
            pltpu.VMEM((8, 8, n), jnp.float32),
            pltpu.VMEM((k, 8 * n), jnp.bfloat16),
            pltpu.VMEM((line, k, n), jnp.float32),
            pltpu.VMEM((line, k, n), jnp.float32),
            pltpu.VMEM((2, 128), jnp.float32),
            pltpu.VMEM((8 * line, 2, 128), jnp.float32),
            dma((8,)), dma((8,)), dma((line + 2,)), dma((line + 2,)), dma((8,)), dma((8,)),
            dma((8,)), dma((8,)), dma((line,)), dma((line,)), dma((8 * line,)), dma((8 * line,)),
        ],
        compiler_params=pltpu.CompilerParams(
            collective_id=0, has_side_effects=True, vmem_limit_bytes=56524800),
        name="cluster",
    )(embeddings.T, vectors.T)
    basis_t, tri = pl.pallas_call(
        store,
        out_shape=(jax.ShapeDtypeStruct((k, n), jnp.float32), jax.ShapeDtypeStruct((k, k), jnp.float32)),
        in_specs=[vmem] * 2,
        out_specs=[pl.BlockSpec(memory_space=pl.ANY)] * 2,
        scratch_shapes=[dma((2,))],
        compiler_params=pltpu.CompilerParams(vmem_limit_bytes=1024 * 1024),
        name="store",
    )(basis_t, tri)
    return basis_t.T, tri


def solution(mesh):
    blk_low = mesh.shape["blk"] // 2
    line = (mesh.shape["row"] // 4) * blk_low
    placed = (P(("row", "blk"), None), P(("row", "blk"), None))
    return jax.shard_map(
        functools.partial(per_device, (blk_low, line)),
        mesh=mesh,
        in_specs=placed,
        out_specs=(P(("row", "blk"), None), P()),
        check_vma=False,
    )
```
